32 devices in a mesh: row: 4 (over x, core), col: 8 (over z, y).
Axes of the slice: x: 2, y: 2, z: 4, core: 2. Of those that a mesh axis runs over, the one named last changes fastest.
Arguments:
- ancestor_inverse: bfloat16 [24576, 24576], P('row', 'col'), may hold values from -0.0390625 to 0.0390625
- panels: bfloat16 [24576, 3, 512], P(('row', 'col')), may hold values from -1.1953125 to 1.1953125
- diag_inverse: float32 [3, 512, 512], replicated, may hold values from -6 to 6
- tile_mask: int32 [3, 192], replicated, may hold values 0 or 1
Outputs:
- off_diagonal: float32 [24576, 3, 512], P(('row', 'col'))
- diagonal: float32 [3, 512, 512], replicated
The draws below stay inside these ranges and needn't reach their ends.
All inputs are finite; a program needn't handle non-finite values.
Results may differ from the reference program's by a relative error of at most 0.0003.
Values may be sent and summed in bfloat16 or wider, within the bound.
A program may use at most 192 MiB of HBM per device.

```python
import jax
import jax.numpy as jnp
from jax import lax

ORDER = 24576
WIDTH = 512
PANELS = 3
TILE = 128


def with_ends(entries, key, smallest, largest):
    index_at = [jax.random.randint(jax.random.fold_in(key, axis), (), 0, length) for axis, length in enumerate(entries.shape)]
    widest = entries.shape.index(max(entries.shape))
    beside = index_at[:widest] + [(index_at[widest] + 1) % entries.shape[widest]] + index_at[widest + 1:]
    return entries.at[tuple(index_at)].set(smallest).at[tuple(beside)].set(largest)


def level_of(rng, extent, pieces, low, top_value):
    level, own = 1.0, jax.random.fold_in(rng, 6)
    for dim, shards_of in pieces:
        heights = jnp.exp(jax.random.uniform(jax.random.fold_in(own, dim), (shards_of,), jnp.float32, low / len(pieces), top_value / len(pieces)))
        level = level * jnp.repeat(heights, extent[dim] // shards_of).reshape([-1 if axis == dim else 1 for axis in range(len(extent))])
    return level


def normal_values(own_key, shape, spread, limit, split=(), held_as=jnp.bfloat16):
    factor_of = level_of(own_key, shape, split, -0.22, 0.18) if split else 1.0
    entries = jax.random.normal(own_key, shape, jnp.float32) * spread * factor_of
    return jnp.minimum(jnp.maximum(entries, -limit), limit).astype(held_as)


def setup_inputs(seed: int = 0) -> dict:
    key_of = jax.random.split(jax.random.key(seed), 5)
    return {
        "ancestor_inverse": normal_values(key_of[0], (ORDER, ORDER), ORDER ** -0.5, 0.0390625, ((0, 4), (1, 8))),
        "panels": normal_values(key_of[1], (ORDER, PANELS, WIDTH), 0.2, 1.1953125, ((0, 32),)),
        "diag_inverse": normal_values(key_of[2], (PANELS, WIDTH, WIDTH), 1.0, 6.0, (), jnp.float32),
        "tile_mask": with_ends((jax.random.randint(key_of[3], (PANELS, ORDER // TILE), 0, 2) < 1).astype(jnp.int32), jax.random.fold_in(key_of[3], 1), 0, 1),
    }


def reference(ancestor_inverse, panels, diag_inverse, tile_mask):
    row_mask = jnp.repeat(tile_mask, TILE, axis=1).T.astype(jnp.bfloat16)
    masked = panels * row_mask[:, :, None]
    flattened = masked.reshape(ORDER, PANELS * WIDTH)
    blocks = ancestor_inverse.reshape(16, ORDER // 16, ORDER)

    def product(block):
        return jnp.dot(block, flattened, preferred_element_type=jnp.float32)

    off_diagonal = -lax.map(product, blocks).reshape(ORDER, PANELS, WIDTH)
    schur = jnp.einsum("mpa,mpb->pab", masked.astype(jnp.float32), off_diagonal, precision=lax.Precision.HIGHEST)
    diagonal = diag_inverse - schur
    return off_diagonal, diagonal
```

```python
import functools

import jax
import jax.numpy as jnp
from jax import lax
from jax.experimental import pallas as pl
from jax.experimental.pallas import tpu as pltpu
from jax.sharding import PartitionSpec as P

MESH = pl.DeviceIdType.MESH
PAD = 16
STEPS = 64.0
TOP = 32000.0


def line_shape(col_count):
    nz = 4 if col_count % 4 == 0 else 1
    return nz, col_count // nz


def peak(value):
    return jnp.max(jnp.abs(value), axis=0, keepdims=True)


def exponent_of(top):
    return jnp.ceil(jnp.log2(jnp.maximum(top, 1e-33)) * STEPS)


def write_codes(ref, start, value, exponent):
    scale = jnp.exp2(exponent * (-1.0 / STEPS)) * TOP
    codes = jnp.round(value * scale).astype(jnp.int32)
    ref[pl.ds(start, value.shape[0]), :] = codes.astype(jnp.int16)


def write_exponent(ref, start, exponent):
    wide = jnp.broadcast_to(exponent, (PAD, exponent.shape[1]))
    ref[pl.ds(start, PAD), :] = wide.astype(jnp.int32).astype(jnp.int16)


def read_scale(ref, start):
    wide = ref[pl.ds(start, PAD), :].astype(jnp.int32).astype(jnp.float32)
    return jnp.exp2(wide[:1] * (1.0 / STEPS)) * (1.0 / TOP)


def read_codes(ref, start, rows, scale):
    return ref[pl.ds(start, rows), :].astype(jnp.int32).astype(jnp.float32) * scale


def kernel(
    dims, a_ref, *refs
):
    nz, ny, rows, parts, panels, slots = dims
    x_refs, refs = refs[:panels], refs[panels:]
    (
    o_ref, xbuf, abuf, qbuf, pbuf, ysend, yrecv, usend, urecv, dsend, drecv, obuf,
    xsem, asem, yssem, yrsem, ussem, ursem, dssem, drsem, osem,
    ) = refs
    count = panels * parts
    r = lax.axis_index("row")
    c = lax.axis_index("col")
    z = c // ny
    y = lax.rem(c, ny)

    def at(zz, yy):
        return (r, zz * ny + yy)

    def a_copy(t, j):
        s = lax.rem(t, parts)
        slot = lax.rem(t * ny + j, 2)
        yy = lax.rem(y + 1 + j, ny)
        return pltpu.make_async_copy(
            a_ref.at[:, yy, pl.ds(pl.multiple_of(s * rows, rows), rows), :], abuf.at[slot], asem.at[slot]
        )

    def x_copy(p):
        return pltpu.make_async_copy(x_refs[p], xbuf.at[p], xsem.at[p])

    def y_copy(t, j):
        yy = lax.rem(y + 1 + j, ny)
        return pltpu.make_async_remote_copy(
            ysend.at[lax.rem(t, 2), j], yrecv.at[t, j], yssem.at[lax.rem(t, 2), j], yrsem.at[t, j],
            device_id=at(z, yy), device_id_type=MESH,
        )

    def line_copy(t, k, send, recv, ssem, rsem, to):
        size = k * rows + PAD
        slot = lax.rem(t, 2)
        return pltpu.make_async_remote_copy(
            send.at[slot, pl.ds(0, size)], recv.at[t, pl.ds(0, size)], ssem.at[slot], rsem.at[t],
            device_id=at(to, y), device_id_type=MESH,
        )

    def up_copy(t, zz):
        return line_copy(t, nz - 1 - zz, usend, urecv, ussem, ursem, lax.rem(z + 1, nz))

    def down_copy(t, zz):
        return line_copy(t, zz, dsend, drecv, dssem, drsem, lax.rem(z + nz - 1, nz))

    def o_copy(t):
        slot = lax.rem(t, 2)
        p = t // parts
        s = lax.rem(t, parts)
        return pltpu.make_async_copy(
            obuf.at[slot], o_ref.at[p, pl.ds(pl.multiple_of(s * rows, rows), rows), :], osem.at[slot]
        )

    for p in range(panels):
        x_copy(p).start()
    a_copy(0, 0).start()
    a_copy(1 // ny, 1 % ny).start()

    barrier = pltpu.get_barrier_semaphore()
    for j in range(ny - 1):
        pl.semaphore_signal(barrier, inc=1, device_id=at(z, lax.rem(y + 1 + j, ny)), device_id_type=MESH)

    @pl.when(z > 0)
    def _():
        pl.semaphore_signal(barrier, inc=1, device_id=at(lax.rem(z + nz - 1, nz), y), device_id_type=MESH)

    @pl.when(z < nz - 1)
    def _():
        pl.semaphore_signal(barrier, inc=1, device_id=at(lax.rem(z + 1, nz), y), device_id_type=MESH)

    pl.semaphore_wait(
        barrier, ny - 1 + jnp.where(z > 0, 1, 0).astype(jnp.int32) + jnp.where(z < nz - 1, 1, 0).astype(jnp.int32)
    )

    def multiply(t, j, out):
        slot = lax.rem(t * ny + j, 2)
        a_copy(t, j).wait()
        p = t // parts
        for i in range(nz):
            out[pl.ds(i * rows, rows), :] = jnp.dot(abuf[slot, i], xbuf[p], preferred_element_type=jnp.float32)

        @pl.when(t * ny + j + 2 < count * ny)
        def _():
            ahead = j + 2
            a_copy(t + ahead // ny, ahead % ny).start()

    def produce(t):
        for p in range(panels):

            @pl.when(t == p * parts)
            def _():
                x_copy(p).wait()

        slot = lax.rem(t, 2)
        for j in range(ny - 1):
            multiply(t, j, pbuf)

            @pl.when(t >= 2)
            def _():
                y_copy(t - 2, j).wait_send()

            exponent = exponent_of(peak(pbuf[...]))
            for i in range(nz):
                write_codes(ysend.at[slot, j], i * rows, pbuf[pl.ds(i * rows, rows), :], exponent)
            write_exponent(ysend.at[slot, j], nz * rows, exponent)
            y_copy(t, j).start()
        multiply(t, ny - 1, qbuf.at[lax.rem(t, slots)])

    def gather(t):
        q = qbuf.at[lax.rem(t, slots)]
        for j in range(ny - 1):
            y_copy(t, j).wait_recv()
            got = yrecv.at[t, j]
            scale = read_scale(got, nz * rows)
            for i in range(nz):
                q[pl.ds(i * rows, rows), :] += read_codes(got, i * rows, rows, scale)

    def pass_on(t, zz, up):
        send, recv, copy = (usend, urecv, up_copy) if up else (dsend, drecv, down_copy)
        toward = 1 if up else -1
        came = nz - zz if up else zz + 1
        first = zz == (0 if up else nz - 1)
        q = qbuf.at[lax.rem(t, slots)]
        if not first:
            copy(t, zz - toward).wait_recv()
        left = came - 1
        if left == 0:
            return

        @pl.when(t >= 2)
        def _():
            copy(t - 2, zz).wait_send()

        top = None
        if not first:
            scale = read_scale(recv.at[t], came * rows)
        for i in range(left):
            block = pl.ds((zz + toward * (i + 1)) * rows, rows)
            value = q[block, :]
            if not first:
                value = value + read_codes(recv.at[t], (i + 1) * rows, rows, scale)
                q[block, :] = value
            top = peak(value) if top is None else jnp.maximum(top, peak(value))
        exponent = exponent_of(top)
        out = send.at[lax.rem(t, 2)]
        for i in range(left):
            block = pl.ds((zz + toward * (i + 1)) * rows, rows)
            write_codes(out, i * rows, q[block, :], exponent)
        write_exponent(out, left * rows, exponent)
        copy(t, zz).start()

    def finish(t, zz):
        q = qbuf.at[lax.rem(t, slots)]

        @pl.when(t >= 2)
        def _():
            o_copy(t - 2).wait()

        value = q[pl.ds(zz * rows, rows), :]
        if zz > 0:
            value = value + read_codes(urecv.at[t], 0, rows, read_scale(urecv.at[t], (nz - zz) * rows))
        if zz < nz - 1:
            value = value + read_codes(drecv.at[t], 0, rows, read_scale(drecv.at[t], (zz + 1) * rows))
        obuf[lax.rem(t, 2)] = -value
        o_copy(t).start()

    def step(t, carry):
        @pl.when(t < count)
        def _():
            produce(t)

        @pl.when((t >= 1) & (t - 1 < count))
        def _():
            gather(t - 1)

        for zz in range(nz):
            for up in (True, False):
                late = t - 1 - (zz if up else nz - 1 - zz)

                @pl.when((z == zz) & (late >= 0) & (late < count))
                def _():
                    pass_on(late, zz, up)

            @pl.when((z == zz) & (t >= nz))
            def _():
                finish(t - nz, zz)

        return carry

    lax.fori_loop(0, count + nz, step, 0)
    for t in (count - 2, count - 1):
        for j in range(ny - 1):
            y_copy(t, j).wait_send()
        for zz in range(nz):

            @pl.when(z == zz)
            def _():
                if zz < nz - 1:
                    up_copy(t, zz).wait_send()
                if zz > 0:
                    down_copy(t, zz).wait_send()

        o_copy(t).wait()


def product(ancestor_inverse, sides, col_count, kept):
    panels = len(sides)
    depth, width = sides[0].shape
    nz, ny = line_shape(col_count)
    rows = max(d for d in range(16, 129, 16) if kept % d == 0)
    parts = kept // rows
    count = panels * parts
    slots = nz + 1
    dims = (nz, ny, rows, parts, panels, slots)
    a = ancestor_inverse.reshape(nz, ny, kept, depth)
    message, line = nz * rows + PAD, (nz - 1) * rows + PAD
    dma = pltpu.SemaphoreType.DMA
    return pl.pallas_call(
        functools.partial(kernel, dims),
        out_shape=jax.ShapeDtypeStruct((panels, kept, width), jnp.float32),
        in_specs=[pl.BlockSpec(memory_space=pl.ANY)] * (1 + panels),
        out_specs=pl.BlockSpec(memory_space=pl.ANY),
        scratch_shapes=[
            pltpu.VMEM((panels, depth, width), jnp.bfloat16),
            pltpu.VMEM((2, nz, rows, depth), jnp.bfloat16),
            pltpu.VMEM((slots, nz * rows, width), jnp.float32),
            pltpu.VMEM((nz * rows, width), jnp.float32),
            pltpu.VMEM((2, ny - 1, message, width), jnp.int16),
            pltpu.VMEM((count, ny - 1, message, width), jnp.int16),
            pltpu.VMEM((2, line, width), jnp.int16),
            pltpu.VMEM((count, line, width), jnp.int16),
            pltpu.VMEM((2, line, width), jnp.int16),
            pltpu.VMEM((count, line, width), jnp.int16),
            pltpu.VMEM((2, rows, width), jnp.float32),
            dma((panels,)), dma((2,)), dma((2, ny - 1)), dma((count, ny - 1)),
            dma((2,)), dma((count,)), dma((2,)), dma((count,)), dma((2,)),
        ],
        compiler_params=pltpu.CompilerParams(
            collective_id=0, has_side_effects=True, vmem_limit_bytes=66_000_000
        ),
        name="product",
    )(a, *sides)


def body(ancestor_inverse, panels, diag_inverse, tile_mask):
    row_count = lax.axis_size("row")
    col_count = lax.axis_size("col")
    span = lax.axis_index("row") * col_count + lax.axis_index("col")
    kept = panels.shape[0]
    panel_count = panels.shape[1]
    tile = kept * row_count * col_count // tile_mask.shape[1]
    full_mask = jnp.repeat(tile_mask, tile, axis=1).astype(jnp.bfloat16)
    own_mask = lax.dynamic_slice_in_dim(full_mask, span * kept, kept, 1)
    moves = [
        (index, (index % row_count) * col_count + index // row_count)
        for index in range(row_count * col_count)
    ]
    masked = jnp.transpose(panels, (1, 0, 2)) * own_mask[:, :, None]
    sent = [lax.ppermute(masked[p], ("row", "col"), moves) for p in range(panel_count)]
    sides = [lax.all_gather(block, "row", axis=0, tiled=True) for block in sent]
    results = product(ancestor_inverse, sides, col_count, kept)
    high = lax.reduce_precision(results, 8, 7)
    low = (results - high).astype(jnp.bfloat16)
    high = high.astype(jnp.bfloat16)

    def pair(part):
        return lax.dot_general(
            masked, part, (((1,), (1,)), ((0,), (0,))), preferred_element_type=jnp.float32
        )

    schur = lax.psum(pair(high) + pair(low), ("row", "col"))
    return jnp.transpose(results, (1, 0, 2)), diag_inverse - schur


def solution(mesh):
    return jax.shard_map(
        body,
        mesh=mesh,
        in_specs=(P("row", "col"), P(("row", "col"), None, None), P(), P()),
        out_specs=(P(("row", "col"), None, None), P()),
        check_vma=False,
    )
```

```python
import functools

import jax
import jax.numpy as jnp
from jax import lax
from jax.experimental import pallas as pl
from jax.experimental.pallas import tpu as pltpu
from jax.sharding import PartitionSpec as P

MESH = pl.DeviceIdType.MESH
PAD = 16
STEPS = 64.0
TOP = 32000.0


def line_shape(col_count):
    nz = 4 if col_count % 4 == 0 else 1
    return nz, col_count // nz


def peak(value):
    return jnp.max(jnp.abs(value), axis=0, keepdims=True)


def exponent_of(top):
    return jnp.ceil(jnp.log2(jnp.maximum(top, 1e-33)) * STEPS)


def write_codes(ref, start, value, exponent):
    scale = jnp.exp2(exponent * (-1.0 / STEPS)) * TOP
    codes = jnp.round(value * scale).astype(jnp.int32)
    ref[pl.ds(start, value.shape[0]), :] = codes.astype(jnp.int16)


def write_exponent(ref, start, exponent):
    wide = jnp.broadcast_to(exponent, (PAD, exponent.shape[1]))
    ref[pl.ds(start, PAD), :] = wide.astype(jnp.int32).astype(jnp.int16)


def read_scale(ref, start):
    wide = ref[pl.ds(start, PAD), :].astype(jnp.int32).astype(jnp.float32)
    return jnp.exp2(wide[:1] * (1.0 / STEPS)) * (1.0 / TOP)


def read_codes(ref, start, rows, scale):
    return ref[pl.ds(start, rows), :].astype(jnp.int32).astype(jnp.float32) * scale


class Several:
    def __init__(self, copies):
        self.copies = list(copies)

    def start(self):
        for copy in self.copies:
            copy.start()

    def wait_send(self):
        for copy in self.copies:
            copy.wait_send()

    def wait_recv(self):
        for copy in self.copies:
            copy.wait_recv()


def kernel(
    dims, a_ref, *refs
):
    nz, ny, nr, rows, parts, panels, slots, whole = dims
    inputs = 1 if whole else panels
    x_refs, refs = refs[:inputs], refs[inputs:]
    if whole:
        o_ref, s_ref, *refs = refs
        own, sbuf, gbuf, rc, rx, ry, rz, x1s, x1r, x2s, x2r, x3s, x3r, ownsem, ss, sr, zs, zr, zs2, zr2, outsem = refs[20:]
        refs = refs[:20]
    else:
        o_ref, *refs = refs
    (
    xbuf, abuf, qbuf, pbuf, ysend, yrecv, usend, urecv, dsend, drecv, obuf,
    xsem, asem, yssem, yrsem, ussem, ursem, dssem, drsem, osem,
    ) = refs
    count = panels * parts
    r = lax.axis_index("row")
    c = lax.axis_index("col")
    z = c // ny
    y = lax.rem(c, ny)

    def at(zz, yy):
        return (r, zz * ny + yy)

    def a_copy(t, j):
        s = lax.rem(t, parts)
        slot = lax.rem(t * ny + j, 2)
        yy = lax.rem(y + 1 + j, ny)
        return pltpu.make_async_copy(
            a_ref.at[:, yy, pl.ds(pl.multiple_of(s * rows, rows), rows), :], abuf.at[slot], asem.at[slot]
        )

    def x_copy(p):
        return pltpu.make_async_copy(x_refs[p], xbuf.at[p], xsem.at[p])

    me = r * (nz * ny) + c
    goal, place = me // nr, lax.rem(me, nr)
    across = lax.rem(r + nr // 2, nr)
    mate = r + 1 - 2 * lax.rem(r, 2)

    def remote(src, dst, ssem, rsem, to):
        return pltpu.make_async_remote_copy(src, dst, ssem, rsem, device_id=to, device_id_type=MESH)

    def own_copy(p):
        return pltpu.make_async_copy(x_refs[0].at[p], own.at[p], ownsem.at[p])

    def deal_copy(p, q):
        size = own.shape[1] // nr
        return remote(
            own.at[p, pl.ds(q * size, size)], xbuf.at[p, place, q], x1s.at[p, q], x1r.at[p, place], (q, goal)
        )

    def deal_wait(p):
        for k in range(nr):

            @pl.when(c * nr + k != me)
            def _():
                spot = xbuf.at[p, k, r]
                remote(spot, spot, x1s.at[p, 0], x1r.at[p, k], (r, c)).wait_recv()

    def across_copy(p, q):
        return Several(
            remote(xbuf.at[p, k, q], xbuf.at[p, k, q], x2s.at[p, k], x2r.at[p, k], (across, c)) for k in range(nr)
        )

    def mate_copy(p, q, i):
        return Several(
            remote(xbuf.at[p, k, q], xbuf.at[p, k, q], x3s.at[p, i, k], x3r.at[p, i, k], (mate, c))
            for k in range(nr)
        )

    def deal(p):
        own_copy(p).wait()
        size = own.shape[1] // nr
        for q in range(nr):
            here = (r == q) & (goal == c)

            @pl.when(jnp.logical_not(here))
            def _():
                deal_copy(p, q).start()

            @pl.when(here)
            def _():
                xbuf[p, place, q] = own[p, pl.ds(q * size, size), :]

    def share(p):
        deal_wait(p)
        across_copy(p, r).start()
        mate_copy(p, r, 0).start()

    def relay(p):
        across_copy(p, across).wait_recv()
        mate_copy(p, across, 1).start()

    def complete(p):
        mate_copy(p, mate, 0).wait_recv()
        mate_copy(p, lax.rem(mate + nr // 2, nr), 1).wait_recv()

    def settle(p):
        for q in range(nr):

            @pl.when(jnp.logical_not((r == q) & (goal == c)))
            def _():
                deal_copy(p, q).wait_send()

        across_copy(p, r).wait_send()
        mate_copy(p, r, 0).wait_send()
        mate_copy(p, across, 1).wait_send()

    def y_copy(t, j):
        yy = lax.rem(y + 1 + j, ny)
        return pltpu.make_async_remote_copy(
            ysend.at[lax.rem(t, 2), j], yrecv.at[t, j], yssem.at[lax.rem(t, 2), j], yrsem.at[t, j],
            device_id=at(z, yy), device_id_type=MESH,
        )

    def line_copy(t, k, send, recv, ssem, rsem, to):
        size = k * rows + PAD
        slot = lax.rem(t, 2)
        return pltpu.make_async_remote_copy(
            send.at[slot, pl.ds(0, size)], recv.at[t, pl.ds(0, size)], ssem.at[slot], rsem.at[t],
            device_id=at(to, y), device_id_type=MESH,
        )

    def up_copy(t, zz):
        return line_copy(t, nz - 1 - zz, usend, urecv, ussem, ursem, lax.rem(z + 1, nz))

    def down_copy(t, zz):
        return line_copy(t, zz, dsend, drecv, dssem, drsem, lax.rem(z + nz - 1, nz))

    def o_copy(t):
        slot = lax.rem(t, 2)
        p = t // parts
        s = lax.rem(t, parts)
        return pltpu.make_async_copy(
            obuf.at[slot], o_ref.at[p, pl.ds(pl.multiple_of(s * rows, rows), rows), :], osem.at[slot]
        )

    for p in range(panels):
        (own_copy if whole else x_copy)(p).start()
    a_copy(0, 0).start()
    a_copy(1 // ny, 1 % ny).start()

    barrier = pltpu.get_barrier_semaphore()
    for j in range(ny - 1):
        pl.semaphore_signal(barrier, inc=1, device_id=at(z, lax.rem(y + 1 + j, ny)), device_id_type=MESH)

    for o in range(1, nz):
        pl.semaphore_signal(barrier, inc=1, device_id=at(lax.rem(z + o, nz), y), device_id_type=MESH)
    if not whole:
        pl.semaphore_wait(barrier, ny + nz - 2)
    else:
        for to in (across, mate):
            pl.semaphore_signal(barrier, inc=1, device_id=(to, c), device_id_type=MESH)
        for k in range(nr):
            origin = c * nr + k

            @pl.when(origin != me)
            def _():
                pl.semaphore_signal(
                    barrier, inc=1, device_id=(origin // (nz * ny), lax.rem(origin, nz * ny)), device_id_type=MESH
                )

        pl.semaphore_wait(barrier, ny + nz + nr - jnp.where(goal == c, 1, 0).astype(jnp.int32))
        deal(0)
        share(0)
        relay(0)

    def multiply(t, j, out):
        slot = lax.rem(t * ny + j, 2)
        a_copy(t, j).wait()
        p = t // parts
        for i in range(nz):
            side = xbuf[p].reshape(abuf.shape[-1], xbuf.shape[-1])
            out[pl.ds(i * rows, rows), :] = jnp.dot(abuf[slot, i], side, preferred_element_type=jnp.float32)

        @pl.when(t * ny + j + 2 < count * ny)
        def _():
            ahead = j + 2
            a_copy(t + ahead // ny, ahead % ny).start()

    def produce(t):
        for p in range(panels):

            @pl.when(t == p * parts)
            def _():
                (complete if whole else lambda q: x_copy(q).wait())(p)

        slot = lax.rem(t, 2)
        for j in range(ny - 1):
            multiply(t, j, pbuf)

            @pl.when(t >= 2)
            def _():
                y_copy(t - 2, j).wait_send()

            exponent = exponent_of(peak(pbuf[...]))
            for i in range(nz):
                write_codes(ysend.at[slot, j], i * rows, pbuf[pl.ds(i * rows, rows), :], exponent)
            write_exponent(ysend.at[slot, j], nz * rows, exponent)
            y_copy(t, j).start()
        multiply(t, ny - 1, qbuf.at[lax.rem(t, slots)])

    def gather(t):
        q = qbuf.at[lax.rem(t, slots)]
        for j in range(ny - 1):
            y_copy(t, j).wait_recv()
            got = yrecv.at[t, j]
            scale = read_scale(got, nz * rows)
            for i in range(nz):
                q[pl.ds(i * rows, rows), :] += read_codes(got, i * rows, rows, scale)

    def pass_on(t, zz, up):
        send, recv, copy = (usend, urecv, up_copy) if up else (dsend, drecv, down_copy)
        toward = 1 if up else -1
        came = nz - zz if up else zz + 1
        first = zz == (0 if up else nz - 1)
        q = qbuf.at[lax.rem(t, slots)]
        if not first:
            copy(t, zz - toward).wait_recv()
        left = came - 1
        if left == 0:
            return

        @pl.when(t >= 2)
        def _():
            copy(t - 2, zz).wait_send()

        top = None
        if not first:
            scale = read_scale(recv.at[t], came * rows)
        for i in range(left):
            block = pl.ds((zz + toward * (i + 1)) * rows, rows)
            value = q[block, :]
            if not first:
                value = value + read_codes(recv.at[t], (i + 1) * rows, rows, scale)
                q[block, :] = value
            top = peak(value) if top is None else jnp.maximum(top, peak(value))
        exponent = exponent_of(top)
        out = send.at[lax.rem(t, 2)]
        for i in range(left):
            block = pl.ds((zz + toward * (i + 1)) * rows, rows)
            write_codes(out, i * rows, q[block, :], exponent)
        write_exponent(out, left * rows, exponent)
        copy(t, zz).start()

    def finish(t, zz):
        q = qbuf.at[lax.rem(t, slots)]

        @pl.when(t >= 2)
        def _():
            o_copy(t - 2).wait()

        value = q[pl.ds(zz * rows, rows), :]
        if zz > 0:
            value = value + read_codes(urecv.at[t], 0, rows, read_scale(urecv.at[t], (nz - zz) * rows))
        if zz < nz - 1:
            value = value + read_codes(drecv.at[t], 0, rows, read_scale(drecv.at[t], (zz + 1) * rows))
        obuf[lax.rem(t, 2)] = -value
        o_copy(t).start()

    if whole:
        half = sbuf.shape[1] // 2
        low = lax.rem(r, 2)
        base1 = low * half
        high = r // 2
        quarter, eighth, bit = half // 2, half // 4, half // (4 * nz)
        base2 = base1 + high * quarter
        base3 = base2 + y * eighth
        base4 = base3 + z * bit

    def g_at(p, start, size):
        return gbuf.at[p, pl.ds(pl.multiple_of(start, 8), size)]

    def s_at(p, start, size):
        return sbuf.at[p, pl.ds(pl.multiple_of(start, 8), size)]

    def swap(p, i):
        to = ((mate, c), (across, c), at(z, lax.rem(y + 1, ny)))[i % 3]
        sems = ss.at[p, i], sr.at[p, i]
        if i < 3:
            size = (half, quarter, eighth)[i]
            start = (half * (1 - low), base1 + quarter * (1 - high), base2 + eighth * (1 - y))[i]
            return remote(s_at(p, start, size), (rc, rx, ry)[i].at[p], *sems, to)
        size, start = ((half, base1), (quarter, base2), (eighth, base3))[i - 3]
        return remote(g_at(p, start, size), g_at(p, start, size), *sems, to)

    def swap_wait(p, i):
        if i < 3:
            swap(p, i).wait_recv()
            size, start = ((half, base1), (quarter, base2), (eighth, base3))[i]
            sbuf[p, pl.ds(pl.multiple_of(start, 8), size), :] += (rc, rx, ry)[i][p]
        else:
            size = (half, quarter, eighth)[i - 3]
            start = (half * (1 - low), base1 + quarter * (1 - high), base2 + eighth * (1 - y))[i - 3]
            spot = g_at(p, start, size)
            remote(spot, spot, ss.at[p, i], sr.at[p, i], (r, c)).wait_recv()

    def spread(p, o, back):
        there = lax.rem(z + o, nz)
        if back:
            return remote(g_at(p, base4, bit), g_at(p, base4, bit), zs2.at[p, o - 1], zr2.at[p, o - 1], at(there, y))
        return remote(
            s_at(p, base3 + there * bit, bit), rz.at[p, o - 1], zs.at[p, o - 1], zr.at[p, o - 1], at(there, y)
        )

    def all_sum(p, i):
        if i == 0:
            swap(p, 0).start()
        elif i <= 2:
            swap_wait(p, i - 1)
            swap(p, i).start()
        elif i == 3:
            swap_wait(p, 2)
            for o in range(1, nz):
                spread(p, o, False).start()
        elif i == 4:
            for o in range(1, nz):
                spread(p, o, False).wait_recv()
            spot = pl.ds(pl.multiple_of(base4, 8), bit)
            total = sbuf[p, spot, :]
            for o in range(1, nz):
                total = total + rz[p, o - 1]
            gbuf[p, spot, :] = total
            for o in range(1, nz):
                spread(p, o, True).start()
        elif i == 5:
            for o in range(1, nz):
                spot = g_at(p, base3 + lax.rem(z - o + nz, nz) * bit, bit)
                remote(spot, spot, zs2.at[p, 0], zr2.at[p, o - 1], (r, c)).wait_recv()
            swap(p, 5).start()
        elif i <= 7:
            swap_wait(p, 11 - i)
            swap(p, 10 - i).start()
        else:
            swap_wait(p, 3)
            for k in range(6):
                swap(p, k).wait_send()
            for o in range(1, nz):
                spread(p, o, False).wait_send()
                spread(p, o, True).wait_send()
            pltpu.make_async_copy(gbuf.at[p], s_ref.at[p], outsem.at[p]).start()

    def pair(t):
        p = t // parts
        s = lax.rem(t, parts)

        @pl.when(s == 0)
        def _():
            sbuf[p] = jnp.zeros(sbuf.shape[1:], jnp.float32)

        value = obuf[lax.rem(t, 2)]
        top = value.astype(jnp.bfloat16)
        rest = (value - top.astype(jnp.float32)).astype(jnp.bfloat16)
        mine = own[p, pl.ds(pl.multiple_of(s * rows, rows), rows), :]
        total = sbuf[p]
        for part in (top, rest):
            total = total + lax.dot_general(
                mine, part, (((0,), (0,)), ((), ())), preferred_element_type=jnp.float32
            )
        sbuf[p] = total

    def step(t, carry):
        if whole:
            for p in range(1, panels):

                @pl.when(t == (p - 1) * parts)
                def _():
                    deal(p)

                @pl.when(t == (p - 1) * parts + 2)
                def _():
                    share(p)

                @pl.when(t == (p - 1) * parts + 4)
                def _():
                    relay(p)

        @pl.when(t < count)
        def _():
            produce(t)

        @pl.when((t >= 1) & (t - 1 < count))
        def _():
            gather(t - 1)

        for zz in range(nz):
            for up in (True, False):
                late = t - 1 - (zz if up else nz - 1 - zz)

                @pl.when((z == zz) & (late >= 0) & (late < count))
                def _():
                    pass_on(late, zz, up)

            @pl.when((z == zz) & (t >= nz) & (t - nz < count))
            def _():
                finish(t - nz, zz)

        if whole:

            @pl.when((t >= nz) & (t - nz < count))
            def _():
                pair(t - nz)

            for i in range(9):
                since = t - (parts + nz - 1) - i

                @pl.when((since >= 0) & (lax.rem(since + parts * 2, parts) == 0) & (since // parts < panels))
                def _():
                    all_sum(since // parts, i)

        return carry

    lax.fori_loop(0, count + nz + (8 if whole else 0), step, 0)
    if whole:
        for p in range(panels):
            settle(p)
            pltpu.make_async_copy(gbuf.at[p], s_ref.at[p], outsem.at[p]).wait()
    for t in (count - 2, count - 1):
        for j in range(ny - 1):
            y_copy(t, j).wait_send()
        for zz in range(nz):

            @pl.when(z == zz)
            def _():
                if zz < nz - 1:
                    up_copy(t, zz).wait_send()
                if zz > 0:
                    down_copy(t, zz).wait_send()

        o_copy(t).wait()


def product(ancestor_inverse, sides, row_count, col_count, kept, panels, whole):
    depth, width = ancestor_inverse.shape[1], sides[0].shape[-1]
    nz, ny = line_shape(col_count)
    rows = max(d for d in range(16, 129, 16) if kept % d == 0)
    parts = kept // rows
    count = panels * parts
    slots = nz + 1
    dims = (nz, ny, row_count, rows, parts, panels, slots, whole)
    a = ancestor_inverse.reshape(nz, ny, kept, depth)
    message, line = nz * rows + PAD, (nz - 1) * rows + PAD
    dma = pltpu.SemaphoreType.DMA
    side = (panels, depth, width)
    outs = [jax.ShapeDtypeStruct((panels, kept, width), jnp.float32)]
    more = []
    if whole:
        side = (panels, row_count, row_count, kept // row_count, width)
        outs.append(jax.ShapeDtypeStruct((panels, width, width), jnp.float32))
        f32 = lambda *shape: pltpu.VMEM((panels, *shape, width), jnp.float32)
        more = [
            pltpu.VMEM((panels, kept, width), jnp.bfloat16),
            f32(width), f32(width), f32(width // 2), f32(width // 4), f32(width // 8), f32(nz - 1, width // (8 * nz)),
            dma((panels, row_count)), dma((panels, row_count)), dma((panels, row_count)), dma((panels, row_count)),
            dma((panels, 2, row_count)), dma((panels, 2, row_count)), dma((panels,)), dma((panels, 6)), dma((panels, 6)),
            dma((panels, nz - 1)), dma((panels, nz - 1)), dma((panels, nz - 1)), dma((panels, nz - 1)),
            dma((panels,)),
        ]
    return pl.pallas_call(
        functools.partial(kernel, dims),
        out_shape=outs,
        in_specs=[pl.BlockSpec(memory_space=pl.ANY)] * (1 + len(sides)),
        out_specs=[pl.BlockSpec(memory_space=pl.ANY)] * len(outs),
        scratch_shapes=[
            pltpu.VMEM(side, jnp.bfloat16),
            pltpu.VMEM((2, nz, rows, depth), jnp.bfloat16),
            pltpu.VMEM((slots, nz * rows, width), jnp.float32),
            pltpu.VMEM((nz * rows, width), jnp.float32),
            pltpu.VMEM((2, ny - 1, message, width), jnp.int16),
            pltpu.VMEM((count, ny - 1, message, width), jnp.int16),
            pltpu.VMEM((2, line, width), jnp.int16),
            pltpu.VMEM((count, line, width), jnp.int16),
            pltpu.VMEM((2, line, width), jnp.int16),
            pltpu.VMEM((count, line, width), jnp.int16),
            pltpu.VMEM((2, rows, width), jnp.float32),
            dma((panels,)), dma((2,)), dma((2, ny - 1)), dma((count, ny - 1)),
            dma((2,)), dma((count,)), dma((2,)), dma((count,)), dma((2,)),
            *more,
        ],
        compiler_params=pltpu.CompilerParams(
            collective_id=0, has_side_effects=True, vmem_limit_bytes=66_000_000
        ),
        name="product",
    )(a, *sides)


def body(ancestor_inverse, panels, diag_inverse, tile_mask):
    row_count = lax.axis_size("row")
    col_count = lax.axis_size("col")
    span = lax.axis_index("row") * col_count + lax.axis_index("col")
    kept = panels.shape[0]
    panel_count = panels.shape[1]
    tile = kept * row_count * col_count // tile_mask.shape[1]
    full_mask = jnp.repeat(tile_mask, tile, axis=1).astype(jnp.bfloat16)
    own_mask = lax.dynamic_slice_in_dim(full_mask, span * kept, kept, 1)
    moves = [
        (index, (index % row_count) * col_count + index // row_count)
        for index in range(row_count * col_count)
    ]
    masked = jnp.transpose(panels, (1, 0, 2)) * own_mask[:, :, None]
    width = panels.shape[2]
    nz, ny = line_shape(col_count)
    whole = row_count == 4 and ny == 2 and nz == 4 and kept % 64 == 0 and kept >= 512 and width % 256 == 0
    if whole:
        results, schur = product(ancestor_inverse, [masked], row_count, col_count, kept, panel_count, True)
        return jnp.transpose(results, (1, 0, 2)), diag_inverse - schur
    sent = [lax.ppermute(masked[p], ("row", "col"), moves) for p in range(panel_count)]
    sides = [lax.all_gather(block, "row", axis=0, tiled=True) for block in sent]
    (results,) = product(ancestor_inverse, sides, row_count, col_count, kept, panel_count, False)
    high = lax.reduce_precision(results, 8, 7)
    low = (results - high).astype(jnp.bfloat16)
    high = high.astype(jnp.bfloat16)

    def pair(part):
        return lax.dot_general(
            masked, part, (((1,), (1,)), ((0,), (0,))), preferred_element_type=jnp.float32
        )

    schur = lax.psum(pair(high) + pair(low), ("row", "col"))
    return jnp.transpose(results, (1, 0, 2)), diag_inverse - schur


def solution(mesh):
    return jax.shard_map(
        body,
        mesh=mesh,
        in_specs=(P("row", "col"), P(("row", "col"), None, None), P(), P()),
        out_specs=(P(("row", "col"), None, None), P()),
        check_vma=False,
    )
```
